512 devices in a mesh: seq: 8 (over z), dp: 64 (over y, x, core).
Axes of the slice: x: 4, y: 8, z: 8, core: 2. Of those that a mesh axis runs over, the one named last changes fastest.
Arguments:
- accept_arrays: bfloat16 [64, 1024, 2048], P('dp', 'seq'), may hold values from -4 to 4
- lookup_arrays: bfloat16 [64, 1024, 2048], P('dp', 'seq'), may hold values from -0.75 to 0.75
- payload_arrays: bfloat16 [64, 1024, 2048], P('dp', 'seq'), may hold values from -6 to 6
- fading_exponent: bfloat16 [64, 1024, 2048], P('dp', 'seq'), may hold values from -14 to 1
- self_boost: float32 [32, 64], replicated, may hold values from -3 to 3
- result_cotangent: bfloat16 [64, 1024, 2048], P('dp', 'seq'), may hold values from -0.75 to 0.75
- initial_memory_matrix: float32 [2048, 64], replicated, may hold values from -12 to 12
Outputs:
- receptance_grad: bfloat16 [64, 1024, 2048], P('dp', 'seq')
- lookup_cotangent: bfloat16 [64, 1024, 2048], P('dp', 'seq')
- value_grad: bfloat16 [64, 1024, 2048], P('dp', 'seq')
- state_grad: float32 [2048, 64], P('dp', 'seq')
The draws below stay inside these ranges and needn't reach their ends.
All inputs are finite; a program needn't handle non-finite values.
Results may differ from the reference program's by a relative error of at most 0.001.
Values sent between devices are 32-bit elements; how exact they have to be, the bound alone decides.
A program may use at most 128 MiB of HBM per device.

```python
import math
import jax
import jax.numpy as jnp
from jax import lax

PARTIAL_UNITS = 32
ATTN_SIZE = 64
TOK_DEV = 128
SEQ_LEN = 1024
BATCH = 64


def draw_fading_exponent(key, part):
    keys = jax.random.split(key, 7)
    shard_count = SEQ_LEN // TOK_DEV
    fast_share = 0.5
    fast = jax.random.uniform(keys[0], (PARTIAL_UNITS, 1)) < fast_share
    slow_rate = jnp.exp(jax.random.uniform(keys[1], (PARTIAL_UNITS, ATTN_SIZE), minval=math.log(0.15), maxval=math.log(0.6))) / SEQ_LEN
    fast_rate = jnp.exp(jax.random.uniform(keys[2], (PARTIAL_UNITS, ATTN_SIZE), minval=math.log(1.0 / 50.0), maxval=math.log(1.0 / 30.0)))
    base = jnp.where(fast, fast_rate, slow_rate)
    shard_factor = jnp.exp(jax.random.uniform(keys[3], (BATCH, shard_count, 1, 1, 1), minval=-0.69, maxval=0.69))
    token_factor = jnp.exp(jax.random.uniform(keys[4], (BATCH, shard_count, TOK_DEV, PARTIAL_UNITS, ATTN_SIZE), minval=-0.69, maxval=0.69))
    decay_rate = (base * shard_factor * token_factor).reshape(BATCH, SEQ_LEN, PARTIAL_UNITS, ATTN_SIZE)
    device_spots = jax.random.randint(keys[5], (BATCH, 2, 1), 0, SEQ_LEN)
    device_places = jnp.arange(SEQ_LEN, dtype=jnp.int32)[None, None, :]
    token_group = jnp.sum((device_places == device_spots).astype(jnp.float32), axis=1)
    loss_value = jax.random.uniform(keys[6], (BATCH, SEQ_LEN, PARTIAL_UNITS, 1), minval=0.2, maxval=0.5)
    decay_rate = decay_rate - token_group[:, :, None, None] * jnp.log(1.0 - loss_value)
    return jnp.log(decay_rate).reshape(BATCH, SEQ_LEN, PARTIAL_UNITS * ATTN_SIZE).astype(jnp.bfloat16)


def raised(drawn, stream_key, source, target, blocks, factor):
    def block_of(axis_at):
        return (jnp.arange(drawn.shape[axis_at]) // (drawn.shape[axis_at] // blocks)).reshape((-1,) + (1,) * (drawn.ndim - 1 - axis_at))

    near = jax.random.permutation(stream_key, blocks)[block_of(target)]
    far = (block_of(target) + blocks // 2) % blocks
    return jnp.where((block_of(source) == near) | (block_of(source) == far), factor * drawn, drawn)


def block_levels(key, shape, cuts, low, top_value):
    factor_of, own = 1.0, jax.random.fold_in(key, 6)
    for axis_at, parts in cuts:
        draws = jnp.exp(jax.random.uniform(jax.random.fold_in(own, axis_at), (parts,), jnp.float32, low / len(cuts), top_value / len(cuts)))
        factor_of = factor_of * jnp.repeat(draws, shape[axis_at] // parts).reshape([-1 if axis == axis_at else 1 for axis in range(len(shape))])
    return factor_of


def centred(key, extent, scale, limit, cuts=(), kind=jnp.bfloat16):
    drawn = scale * jax.random.normal(key, extent, jnp.float32)
    if cuts:
        drawn = drawn * block_levels(key, extent, cuts, -0.22, 0.18)
    return jnp.clip(drawn, -limit, limit).astype(kind)


def noise_with(own_key, dims, width, reach, cuts, heavy, held_as=jnp.bfloat16):
    entries = width * jax.random.normal(own_key, dims, jnp.float32)
    if cuts:
        entries = entries * block_levels(own_key, dims, cuts, -0.22, 0.18)
    return jnp.clip(raised(entries, jax.random.fold_in(own_key, 3), *heavy), -reach, reach).astype(held_as)


def setup_inputs(seed: int = 0) -> dict:
    arg_keys = jax.random.split(jax.random.key(seed), 8)
    accept_arrays = noise_with(arg_keys[0], (BATCH, SEQ_LEN, PARTIAL_UNITS * ATTN_SIZE), 0.25, 4.0, ((0, 64), (1, 8)), (0, 2, 64, 4.0))
    lookup_arrays = centred(arg_keys[1], (BATCH, SEQ_LEN, PARTIAL_UNITS * ATTN_SIZE), 0.125, 0.75, ((0, 64), (1, 8)))
    payload_arrays = centred(arg_keys[2], (BATCH, SEQ_LEN, PARTIAL_UNITS * ATTN_SIZE), 1.0, 6.0, ((0, 64), (1, 8)))
    fading_exponent = draw_fading_exponent(jax.random.fold_in(arg_keys[7], 71), 0)
    self_boost = centred(arg_keys[4], (PARTIAL_UNITS, ATTN_SIZE), 1.0, 3.0, (), jnp.float32)
    result_cotangent = centred(arg_keys[5], (BATCH, SEQ_LEN, PARTIAL_UNITS * ATTN_SIZE), 0.125, 0.75, ((0, 64), (1, 8)))
    initial_memory_matrix = centred(arg_keys[6], (PARTIAL_UNITS * ATTN_SIZE, ATTN_SIZE), 2.0, 12.0, (), jnp.float32)
    return {"accept_arrays": accept_arrays, "lookup_arrays": lookup_arrays, "payload_arrays": payload_arrays, "fading_exponent": fading_exponent, "self_boost": self_boost, "result_cotangent": result_cotangent, "initial_memory_matrix": initial_memory_matrix}


def split_heads(array):
    return array.astype(jnp.float32).reshape(BATCH, SEQ_LEN, PARTIAL_UNITS, ATTN_SIZE).transpose(1, 0, 2, 3)


def merge_heads(array):
    return array.transpose(1, 0, 2, 3).reshape(BATCH, SEQ_LEN, PARTIAL_UNITS * ATTN_SIZE).astype(jnp.bfloat16)


def reference(accept_arrays, lookup_arrays, payload_arrays, fading_exponent, self_boost, result_cotangent, initial_memory_matrix):
    accept_matrix_lines = split_heads(accept_arrays)
    lookup_matrix_slice = split_heads(lookup_arrays)
    val_rows = split_heads(payload_arrays)
    grad_rows = split_heads(result_cotangent)
    decays = jnp.exp(-jnp.exp(split_heads(fading_exponent)))
    finest_accuracy = lax.Precision.HIGHEST
    start = jnp.broadcast_to(initial_memory_matrix.astype(jnp.float32).reshape(PARTIAL_UNITS, ATTN_SIZE, ATTN_SIZE), (BATCH, PARTIAL_UNITS, ATTN_SIZE, ATTN_SIZE))

    def forward(evolving_memory, inputs):
        present_accept, present_lookup, present_payload, dec_now, present_cotangent = inputs
        scalar_dotted = jnp.sum(present_payload * present_cotangent, axis=-1, keepdims=True)
        accept_cotangent = jnp.einsum("dcpu,dcu->dcp", evolving_memory, present_cotangent, precision=finest_accuracy) + self_boost * present_lookup * scalar_dotted
        evolving_memory = dec_now[..., None] * evolving_memory + present_lookup[..., None] * present_payload[..., None, :]
        return evolving_memory, accept_cotangent

    _, rec_grads = lax.scan(forward, start, (accept_matrix_lines, lookup_matrix_slice, val_rows, decays, grad_rows))

    def backward(scan_memory, inputs):
        present_accept, present_lookup, present_payload, dec_now, present_cotangent = inputs
        scalar_dotted = jnp.sum(present_payload * present_cotangent, axis=-1, keepdims=True)
        fading_factor = jnp.sum(present_accept * self_boost * present_lookup, axis=-1, keepdims=True)
        lookup_cotangent = jnp.einsum("dcpu,dcu->dcp", scan_memory, present_payload, precision=finest_accuracy) + present_accept * self_boost * scalar_dotted
        val_grad = jnp.einsum("bhij,bhi->bhj", scan_memory, present_lookup, precision=finest_accuracy) + fading_factor * present_cotangent
        scan_memory = dec_now[..., None] * scan_memory + present_accept[..., None] * present_cotangent[..., None, :]
        return scan_memory, (lookup_cotangent, val_grad)

    zeros = jnp.zeros((BATCH, PARTIAL_UNITS, ATTN_SIZE, ATTN_SIZE), jnp.float32)
    final, (key_grads, val_grads) = lax.scan(backward, zeros, (accept_matrix_lines, lookup_matrix_slice, val_rows, decays, grad_rows), reverse=True)
    state_grad = jnp.sum(final, axis=0).reshape(PARTIAL_UNITS * ATTN_SIZE, ATTN_SIZE)
    return merge_heads(rec_grads), merge_heads(key_grads), merge_heads(val_grads), state_grad
```

```python
import functools

import jax
import jax.numpy as jnp
from jax import lax
from jax.experimental import pallas as pl
from jax.experimental.pallas import tpu as pltpu
from jax.sharding import PartitionSpec as P

F32 = jnp.float32
BF16 = jnp.bfloat16
LANES = 128
BLOCK = 32


def dot_nn(a, b):
    return lax.dot_general(a, b, (((1,), (0,)), ((), ())), preferred_element_type=F32)


def dot_nt(a, b):
    return lax.dot_general(a, b, (((1,), (1,)), ((), ())), preferred_element_type=F32)


def dot_tn(a, b):
    return lax.dot_general(a, b, (((0,), (0,)), ((), ())), preferred_element_type=F32)


def halves(x):
    hi = x.astype(BF16)
    return hi, (x - hi.astype(F32)).astype(BF16)


def thirds(x):
    hi = x.astype(BF16)
    rest = x - hi.astype(F32)
    mid = rest.astype(BF16)
    return hi, mid, (rest - mid.astype(F32)).astype(BF16)


def iota2(shape, dim):
    return lax.broadcasted_iota(jnp.int32, shape, dim)


def per_head(x):
    first = iota2(x.shape, 1) < LANES // 2
    zero = jnp.zeros_like(x)
    return jnp.concatenate([jnp.where(first, x, zero), jnp.where(first, zero, x)], axis=0)


def per_head_halves(x):
    hi, lo = halves(per_head(x))
    return jnp.concatenate([hi, lo], axis=1)


def folded(x):
    return x[:, :LANES] + x[:, LANES:]


def rows_of(parts):
    return jnp.concatenate([jnp.broadcast_to(p, (BLOCK, LANES)) for p in parts], axis=0)


def decays(f_ref, at):
    tok = f_ref.shape[0]
    log_w = -jnp.exp(f_ref[:, at].astype(F32))
    row, col = iota2((tok, tok), 0), iota2((tok, tok), 1)
    tri = jnp.where((col <= row) & (col // BLOCK == row // BLOCK), 1.0, 0.0).astype(BF16)
    hi, mid, lo = thirds(log_w)
    sums = dot_nn(tri, jnp.concatenate([hi, mid, lo], axis=1))
    upto = sums[:, :LANES] + (sums[:, LANES : 2 * LANES] + sums[:, 2 * LANES :])
    return upto, upto - log_w


def totals_of(upto):
    return [upto[b * BLOCK + BLOCK - 1 : (b + 1) * BLOCK] for b in range(upto.shape[0] // BLOCK)]


def phase_one(i, refs):
    at = pl.ds(pl.multiple_of(i * LANES, LANES), LANES)
    upto, before = decays(refs["f"], at)
    t = totals_of(upto)
    zero = jnp.zeros_like(t[0])
    early = jnp.exp(before + rows_of([zero, t[0], t[0] + t[1], t[0] + t[1] + t[2]]))
    tail = jnp.exp(rows_of([t[0] + t[1] + t[2] + t[3], t[1] + t[2] + t[3], t[2] + t[3], t[3]]) - upto)
    refs["upto"][:, at] = upto
    refs["before"][:, at] = before
    refs["early"][:, at] = early
    refs["tail"][:, at] = tail
    refs["decay"][:, at] = jnp.exp(t[0] + t[1] + t[2] + t[3])
    first = iota2((LANES // 2, LANES), 1) < LANES // 2

    def increment(x, scaled):
        hi, lo = halves(scaled)
        both = folded(dot_tn(x, jnp.concatenate([hi, lo], axis=1)))
        return jnp.where(first, both[: LANES // 2], both[LANES // 2 :])

    refs["state"][:, at] = increment(refs["v"][:, at], refs["k"][:, at].astype(F32) * tail)
    refs["grad"][:, at] = increment(refs["dy"][:, at], refs["r"][:, at].astype(F32) * early)


def phase_two(i, refs):
    at = pl.ds(pl.multiple_of(i * LANES, LANES), LANES)
    r, k = refs["r"][:, at].astype(F32), refs["k"][:, at].astype(F32)
    v, dy = refs["v"][:, at], refs["dy"][:, at]
    upto, before = refs["upto"][:, at], refs["before"][:, at]
    tok = r.shape[0]
    t = totals_of(upto)
    zero = jnp.zeros_like(t[0])
    whole = rows_of(t)
    half = 0.5 * whole
    v_heads, dy_heads = per_head(v), per_head(dy)
    scores = halves(dot_nt(dy, v_heads))
    scores_t = halves(dot_nt(v, dy_heads))
    row = iota2((tok, 2 * tok), 0)
    col = iota2((tok, 2 * tok), 1) % tok
    early_1, tail_1 = jnp.exp(before), jnp.exp(whole - upto)
    levels = [
        (jnp.exp(before - half), jnp.exp(half - upto), lambda a, b: (b < a) & (a // BLOCK == b // BLOCK)),
        (
            early_1,
            tail_1,
            lambda a, b: (b // BLOCK < a // BLOCK) & (a // (2 * BLOCK) == b // (2 * BLOCK)),
        ),
        (
            early_1 * jnp.exp(rows_of([zero, zero, zero, t[2]])),
            tail_1 * jnp.exp(rows_of([t[1], zero, zero, zero])),
            lambda a, b: b // (2 * BLOCK) < a // (2 * BLOCK),
        ),
    ]
    rec = jnp.zeros((tok, LANES), F32)
    key = jnp.zeros((tok, LANES), F32)
    cross = jnp.zeros((tok, 2 * tok), F32)
    none = jnp.zeros((tok, 2 * tok), BF16)
    for r_scale, k_scale, inside in levels:
        lower, upper = inside(row, col), inside(col, row)
        r_heads = per_head_halves(r * r_scale)
        k_level = k * k_scale
        k_heads = per_head_halves(k_level)
        k_hi, k_lo = halves(k_level)
        rec_level = folded(dot_nn(jnp.where(lower, scores[0], none), k_heads))
        rec_level += dot_nn(jnp.where(lower, scores[1], none), k_heads[:, :LANES])
        rec += rec_level * r_scale
        key_level = folded(dot_nn(jnp.where(upper, scores_t[0], none), r_heads))
        key_level += dot_nn(jnp.where(upper, scores_t[1], none), r_heads[:, :LANES])
        key += key_level * k_scale
        cross_level = dot_nt(k_hi, r_heads[:, :LANES]) + (
            dot_nt(k_hi, r_heads[:, LANES:]) + dot_nt(k_lo, r_heads[:, :LANES])
        )
        cross += jnp.where(upper, cross_level, 0.0)
    cross_hi, cross_lo = halves(cross)
    val = dot_nn(cross_hi, dy_heads) + dot_nn(cross_lo, dy_heads)
    boost = refs["u"][:, at]
    same = (iota2((LANES, LANES), 0) < LANES // 2) == (iota2((LANES, LANES), 1) < LANES // 2)
    ones = jnp.where(same, 1.0, 0.0).astype(BF16)
    dy_f = dy.astype(F32)
    own_r, own_k = r * boost, k * boost
    vd_hi, vd_lo = halves(v.astype(F32) * dy_f)
    rk_hi, rk_lo = halves(own_r * k)
    scalar = dot_nn(vd_hi, ones) + dot_nn(vd_lo, ones)
    factor = dot_nn(rk_hi, ones) + dot_nn(rk_lo, ones)
    refs["rec"][:, at] = rec + own_k * scalar
    refs["key"][:, at] = key + own_r * scalar
    refs["val"][:, at] = val + factor * dy_f


def phase_three(i, refs):
    at = pl.ds(pl.multiple_of(i * LANES, LANES), LANES)
    v, dy = refs["v"][:, at], refs["dy"][:, at]
    early, tail = refs["early"][:, at], refs["tail"][:, at]
    state_in = per_head_halves(refs["state_in"][:, at])
    grad_in = per_head_halves(refs["grad_in"][:, at])
    grad_hi, grad_lo = grad_in[:, :LANES], grad_in[:, LANES:]
    k_hi, k_lo = halves(refs["k"][:, at].astype(F32) * tail)
    rec = refs["rec"][:, at] + early * folded(dot_nn(dy, state_in))
    key = refs["key"][:, at] + tail * folded(dot_nn(v, grad_in))
    val = refs["val"][:, at] + (dot_nt(k_hi, grad_hi) + (dot_nt(k_hi, grad_lo) + dot_nt(k_lo, grad_hi)))
    refs["rec_out"][:, at] = rec.astype(BF16)
    refs["key_out"][:, at] = key.astype(BF16)
    refs["val_out"][:, at] = val.astype(BF16)


ONE = ("r", "k", "v", "f", "u", "dy")
ONE_OUT = ("state", "grad", "decay", "rec", "key", "val", "early", "tail")


def kernel_one(pairs, *refs):
    named = dict(zip(ONE + ONE_OUT + ("upto", "before"), refs))
    lax.fori_loop(0, pairs, lambda i, c: (phase_one(i, named), c)[1], 0)
    lax.fori_loop(0, pairs, lambda i, c: (phase_two(i, named), c)[1], 0)


TWO = ("k", "v", "dy", "rec", "key", "val", "early", "tail", "state_in", "grad_in")


def kernel_two(pairs, *refs):
    named = dict(zip(TWO + ("rec_out", "key_out", "val_out"), refs))
    lax.fori_loop(0, pairs, lambda i, c: (phase_three(i, named), c)[1], 0)


def local_part(r, k, v, f, u, dy):
    tok, width = r.shape
    half = LANES // 2
    shapes = [(half, width)] * 2 + [(1, width)] + [(tok, width)] * 5
    return pl.pallas_call(
        functools.partial(kernel_one, width // LANES),
        out_shape=[jax.ShapeDtypeStruct(s, F32) for s in shapes],
        in_specs=[pl.BlockSpec(memory_space=pltpu.VMEM)] * 6,
        out_specs=[pl.BlockSpec(memory_space=pltpu.VMEM)] * 8,
        scratch_shapes=[pltpu.VMEM((tok, width), F32)] * 2,
        compiler_params=pltpu.CompilerParams(vmem_limit_bytes=48 << 20),
        cost_estimate=pl.CostEstimate(flops=1 << 31, bytes_accessed=8 << 20, transcendentals=0),
    )(r, k, v, f, u, dy)


def last_part(k, v, dy, rec, key, val, early, tail, state_in, grad_in):
    tok, width = k.shape
    return pl.pallas_call(
        functools.partial(kernel_two, width // LANES),
        out_shape=[jax.ShapeDtypeStruct((tok, width), BF16)] * 3,
        in_specs=[pl.BlockSpec(memory_space=pltpu.VMEM)] * 10,
        out_specs=[pl.BlockSpec(memory_space=pltpu.VMEM)] * 3,
        compiler_params=pltpu.CompilerParams(vmem_limit_bytes=48 << 20),
        cost_estimate=pl.CostEstimate(flops=1 << 29, bytes_accessed=8 << 20, transcendentals=0),
    )(k, v, dy, rec, key, val, early, tail, state_in, grad_in)


def carried(decay, value, start, axis, reverse):
    count, position = lax.axis_size(axis), lax.axis_index(axis)
    decay_all, value_all = lax.all_gather(decay, axis), lax.all_gather(value, axis)
    total, product = start, jnp.ones_like(decay)
    for n in range(count):
        at = count - 1 - n if reverse else n
        reached = at > position if reverse else at < position
        total = jnp.where(reached, decay_all[at] * total + value_all[at], total)
        product = jnp.where(reached, decay_all[at] * product, product)
    return product, total


def sent_and_summed(value, axis):
    arrived = lax.all_to_all(value, axis, split_axis=0, concat_axis=0, tiled=True)
    return arrived.sum(axis=0)


def on_device(r, k, v, f, u, dy, initial):
    batch, tok, width = r.shape
    heads, size = u.shape
    r, k, v, f, dy = (x.reshape(tok, width) for x in (r, k, v, f, dy))
    state, grad, decay, rec, key, val, early, tail = local_part(r, k, v, f, u.reshape(1, width), dy)
    prefix, state_in = carried(decay, state, initial.T, "seq", False)
    _, grad_in = carried(decay, grad, jnp.zeros_like(grad), "seq", True)
    outs = last_part(k, v, dy, rec, key, val, early, tail, state_in, grad_in)
    dp, seq = lax.axis_size("dp"), lax.axis_size("seq")
    term = (prefix * grad).reshape(size, dp, width // dp).transpose(1, 0, 2)
    summed = sent_and_summed(term.reshape(dp, size * width // dp // LANES, LANES), "dp")
    summed = sent_and_summed(summed.reshape(seq, size * width // dp // seq), "seq")
    state_grad = summed.reshape(size // seq, width // dp).T
    return tuple(x.reshape(batch, tok, width) for x in outs) + (state_grad,)


def solution(mesh):
    rows = P("dp", "seq", None)
    return jax.shard_map(
        on_device,
        mesh=mesh,
        in_specs=(rows, rows, rows, rows, P(), rows, P()),
        out_specs=(rows, rows, rows, P("dp", "seq")),
        check_vma=False,
    )
```

```python
import functools

import jax
import jax.numpy as jnp
from jax import lax
from jax.experimental import pallas as pl
from jax.experimental.pallas import tpu as pltpu
from jax.sharding import PartitionSpec as P

F32 = jnp.float32
BF16 = jnp.bfloat16
LANES = 128
BLOCK = 32


def dot_nn(a, b):
    return lax.dot_general(a, b, (((1,), (0,)), ((), ())), preferred_element_type=F32)


def dot_nt(a, b):
    return lax.dot_general(a, b, (((1,), (1,)), ((), ())), preferred_element_type=F32)


def dot_tn(a, b):
    return lax.dot_general(a, b, (((0,), (0,)), ((), ())), preferred_element_type=F32)


def halves(x):
    hi = x.astype(BF16)
    return hi, (x - hi.astype(F32)).astype(BF16)


def thirds(x):
    hi = x.astype(BF16)
    rest = x - hi.astype(F32)
    mid = rest.astype(BF16)
    return hi, mid, (rest - mid.astype(F32)).astype(BF16)


def iota2(shape, dim):
    return lax.broadcasted_iota(jnp.int32, shape, dim)


def per_head(x):
    first = iota2(x.shape, 1) < LANES // 2
    zero = jnp.zeros_like(x)
    return jnp.concatenate([jnp.where(first, x, zero), jnp.where(first, zero, x)], axis=0)


def per_head_halves(x):
    hi, lo = halves(per_head(x))
    return jnp.concatenate([hi, lo], axis=1)


def folded(x):
    return x[:, :LANES] + x[:, LANES:]


def rows_of(parts):
    return jnp.concatenate([jnp.broadcast_to(p, (BLOCK, LANES)) for p in parts], axis=0)


def decays(f_ref, at):
    tok = f_ref.shape[0]
    log_w = -jnp.exp(f_ref[:, at].astype(F32))
    row, col = iota2((tok, tok), 0), iota2((tok, tok), 1)
    tri = jnp.where((col <= row) & (col // BLOCK == row // BLOCK), 1.0, 0.0).astype(BF16)
    hi, mid, lo = thirds(log_w)
    sums = dot_nn(tri, jnp.concatenate([hi, mid, lo], axis=1))
    upto = sums[:, :LANES] + (sums[:, LANES : 2 * LANES] + sums[:, 2 * LANES :])
    return upto, upto - log_w


def totals_of(upto):
    return [upto[b * BLOCK + BLOCK - 1 : (b + 1) * BLOCK] for b in range(upto.shape[0] // BLOCK)]


def shard_sums(upto):
    t = totals_of(upto)
    zero = jnp.zeros_like(t[0])
    ahead = [zero, t[0], t[0] + t[1], t[0] + t[1] + t[2]]
    behind = [t[1] + t[2] + t[3], t[2] + t[3], t[3], zero]
    return t, ahead, behind, t[0] + behind[0]


def lanes_at(i):
    return pl.ds(pl.multiple_of(i * LANES, LANES), LANES)


def phase_one(i, refs):
    at = lanes_at(i)
    upto, before = decays(refs["f"], at)
    t, ahead, behind, everything = shard_sums(upto)
    early = jnp.exp(before + rows_of(ahead))
    tail = jnp.exp(rows_of([a + b for a, b in zip(t, behind)]) - upto)
    refs["upto"][:, at] = upto
    refs["before"][:, at] = before
    refs["early"][:, at] = early
    refs["tail"][:, at] = tail
    refs["decay"][pl.ds(i, 1), :] = jnp.exp(everything)
    first = iota2((LANES // 2, LANES), 1) < LANES // 2

    def increment(x, scaled):
        hi, lo = halves(scaled)
        both = folded(dot_tn(x, jnp.concatenate([hi, lo], axis=1)))
        return jnp.where(first, both[: LANES // 2], both[LANES // 2 :])

    refs["state"][i] = increment(refs["v"][:, at], refs["k"][:, at].astype(F32) * tail)
    refs["grad"][i] = increment(refs["dy"][:, at], refs["r"][:, at].astype(F32) * early)


def phase_two(i, refs):
    at = lanes_at(i)
    r, k = refs["r"][:, at].astype(F32), refs["k"][:, at].astype(F32)
    v, dy = refs["v"][:, at], refs["dy"][:, at]
    upto, before = refs["upto"][:, at], refs["before"][:, at]
    tok = r.shape[0]
    t = totals_of(upto)
    zero = jnp.zeros_like(t[0])
    whole = rows_of(t)
    half = 0.5 * whole
    v_heads, dy_heads = per_head(v), per_head(dy)
    scores = halves(dot_nt(dy, v_heads))
    scores_t = halves(dot_nt(v, dy_heads))
    row = iota2((tok, 2 * tok), 0)
    col = iota2((tok, 2 * tok), 1) % tok
    early_1, tail_1 = jnp.exp(before), jnp.exp(whole - upto)
    levels = [
        (jnp.exp(before - half), jnp.exp(half - upto), lambda a, b: (b < a) & (a // BLOCK == b // BLOCK)),
        (
            early_1,
            tail_1,
            lambda a, b: (b // BLOCK < a // BLOCK) & (a // (2 * BLOCK) == b // (2 * BLOCK)),
        ),
        (
            early_1 * jnp.exp(rows_of([zero, zero, zero, t[2]])),
            tail_1 * jnp.exp(rows_of([t[1], zero, zero, zero])),
            lambda a, b: b // (2 * BLOCK) < a // (2 * BLOCK),
        ),
    ]
    rec = jnp.zeros((tok, LANES), F32)
    key = jnp.zeros((tok, LANES), F32)
    cross = jnp.zeros((tok, 2 * tok), F32)
    none = jnp.zeros((tok, 2 * tok), BF16)
    for r_scale, k_scale, inside in levels:
        lower, upper = inside(row, col), inside(col, row)
        r_heads = per_head_halves(r * r_scale)
        k_level = k * k_scale
        k_heads = per_head_halves(k_level)
        k_hi, k_lo = halves(k_level)
        rec_level = folded(dot_nn(jnp.where(lower, scores[0], none), k_heads))
        rec_level += dot_nn(jnp.where(lower, scores[1], none), k_heads[:, :LANES])
        rec += rec_level * r_scale
        key_level = folded(dot_nn(jnp.where(upper, scores_t[0], none), r_heads))
        key_level += dot_nn(jnp.where(upper, scores_t[1], none), r_heads[:, :LANES])
        key += key_level * k_scale
        cross_level = dot_nt(k_hi, r_heads[:, :LANES]) + (
            dot_nt(k_hi, r_heads[:, LANES:]) + dot_nt(k_lo, r_heads[:, :LANES])
        )
        cross += jnp.where(upper, cross_level, 0.0)
    cross_hi, cross_lo = halves(cross)
    val = dot_nn(cross_hi, dy_heads) + dot_nn(cross_lo, dy_heads)
    boost = jnp.concatenate([refs["u"][pl.ds(2 * i, 1), :], refs["u"][pl.ds(2 * i + 1, 1), :]], axis=1)
    same = (iota2((LANES, LANES), 0) < LANES // 2) == (iota2((LANES, LANES), 1) < LANES // 2)
    ones = jnp.where(same, 1.0, 0.0).astype(BF16)
    dy_f = dy.astype(F32)
    own_r, own_k = r * boost, k * boost
    vd_hi, vd_lo = halves(v.astype(F32) * dy_f)
    rk_hi, rk_lo = halves(own_r * k)
    scalar = dot_nn(vd_hi, ones) + dot_nn(vd_lo, ones)
    factor = dot_nn(rk_hi, ones) + dot_nn(rk_lo, ones)
    refs["rec"][:, at] = rec + own_k * scalar
    refs["key"][:, at] = key + own_r * scalar
    refs["val"][:, at] = val + factor * dy_f


def phase_three(i, refs):
    at = lanes_at(i)
    v, dy = refs["v"][:, at], refs["dy"][:, at]
    early, tail = refs["early"][:, at], refs["tail"][:, at]
    state_in = per_head_halves(refs["state_in"][i])
    grad_in = per_head_halves(refs["grad_in"][i])
    grad_hi, grad_lo = grad_in[:, :LANES], grad_in[:, LANES:]
    k_hi, k_lo = halves(refs["k"][:, at].astype(F32) * tail)
    rec = refs["rec"][:, at] + early * folded(dot_nn(dy, state_in))
    key = refs["key"][:, at] + tail * folded(dot_nn(v, grad_in))
    val = refs["val"][:, at] + (dot_nt(k_hi, grad_hi) + (dot_nt(k_hi, grad_lo) + dot_nt(k_lo, grad_hi)))
    refs["rec_done"][:, at] = rec.astype(BF16)
    refs["key_done"][:, at] = key.astype(BF16)
    refs["val_done"][:, at] = val.astype(BF16)


X_SIZE = 4
HOP = 3
TERM_AT, CORE_AT, X_AT, Y_AT, Z_AT, LAST_AT = 5, 7, 13, 19, 26, 30

OUT = ("rec_out", "key_out", "val_out", "state_grad")


def kernel(seq_size, dp_size, names, *all_refs):
    g = dict(zip(names, all_refs))
    pairs = g["state"].shape[0]
    half = LANES // 2
    x_size, y_size = X_SIZE, dp_size // (2 * X_SIZE)
    z, d = lax.axis_index("seq"), lax.axis_index("dp")
    c = d % 2
    x = (d // 2) % x_size
    y = d // (2 * x_size)
    last = seq_size - 1

    def chip(x_at, y_at, c_at):
        return {"dp": (y_at * x_size + x_at) * 2 + c_at}

    barrier = pltpu.get_barrier_semaphore()
    peers = [{"seq": (z + n) % seq_size} for n in range(1, seq_size)]
    peers += [chip((x + n) % x_size, y, c) for n in range(1, x_size)]
    peers += [chip(x, (y + n) % y_size, c) for n in range(1, y_size)]
    peers += [chip(x, y, 1 - c)]
    for peer in peers:
        pl.semaphore_signal(barrier, inc=1, device_id=peer, device_id_type=pl.DeviceIdType.MESH)

    loads = [
        pltpu.make_async_copy(g[n + "_hbm"], g[n], g["load_sem"].at[at]) for at, n in enumerate(("f", "k", "v", "r", "dy"))
    ]
    for load in loads:
        load.start()
    load_initial = pltpu.make_async_copy(g["initial_hbm"], g["initial"], g["load_sem"].at[5])

    @pl.when(z == 0)
    def _():
        load_initial.start()

    def remote(src, dst, send, recv, to):
        return pltpu.make_async_remote_copy(
            src_ref=src, dst_ref=dst, send_sem=send, recv_sem=recv, device_id=to, device_id_type=pl.DeviceIdType.MESH
        )

    def forward(j):
        to = {"seq": (z + 1) % seq_size}
        return remote(g["state_out"].at[j], g["state_in"].at[j], g["fs"].at[j], g["fr"].at[j], to)

    def backward(j):
        to = {"seq": (z + last) % seq_size}
        return remote(g["grad_out"].at[j], g["grad_in"].at[j], g["bs"].at[j], g["br"].at[j], to)

    def forward_on(j):
        g["state_out"][j] = g["decay"][pl.ds(j, 1), :] * g["state_in"][j] + g["state"][j]
        forward(j).start()

    def backward_on(j):
        g["grad_out"][j] = g["decay"][pl.ds(j, 1), :] * g["grad_in"][j] + g["grad"][j]
        backward(j).start()

    for load in loads:
        load.wait()

    @pl.when(z == 0)
    def _():
        load_initial.wait()

    pl.semaphore_wait(barrier, len(peers))

    def start_step(i, carry):
        phase_one(i, g)

        @pl.when(z == 0)
        def _():
            g["state_in"][i] = g["initial"][:, lanes_at(i)]
            forward_on(i)

        @pl.when(z == last)
        def _():
            g["grad_in"][i] = jnp.zeros((half, LANES), F32)
            backward_on(i)

        return carry

    lax.fori_loop(0, pairs, start_step, 0)

    def decay_to(n):
        return remote(g["decay"], g["decays"].at[z], g["ds"].at[n - 1], g["dr"].at[z], {"seq": (z + n) % seq_size})

    for n in range(1, seq_size):

        @pl.when(z + n <= last)
        def _():
            decay_to(n).start()

    def core_copy():
        return remote(
            g["term"].at[:, :, pl.ds(pl.multiple_of(16 * (1 - c), 16), 16)],
            g["core_in"],
            g["cs"].at[0],
            g["cr"].at[0],
            chip(x, y, 1 - c),
        )

    def x_copy(n):
        to = (x + n) % x_size
        return remote(g["summed"].at[:, to], g["x_in"].at[n - 1], g["xs"].at[n - 1], g["xr"].at[n - 1], chip(to, y, c))

    def y_copy(n):
        to = (y + n) % y_size
        return remote(g["x_sum"].at[to], g["y_in"].at[n - 1], g["ys"].at[n - 1], g["yr"].at[n - 1], chip(x, to, c))

    def z_copy(n):
        b, hi = n % 2, n // 2
        to = 2 * c + b + 4 * hi
        return to, remote(g["y_sum"].at[pl.ds(8 * b, 8)], g["z_in"].at[z], g["zs"].at[n], g["zr"].at[z], {"seq": to})

    def last_copy():
        return remote(g["z_sum"], g["z_other"], g["cs"].at[1], g["cr"].at[1], chip(x, y, 1 - c))

    gathers = (z % 4) // 2 == c

    def make_terms():
        g["prefix"][...] = jnp.ones((pairs, LANES), F32)
        for q in range(last):

            @pl.when(q < z)
            def _():
                remote(g["decay"], g["decays"].at[q], g["ds"].at[0], g["dr"].at[q], {"seq": z}).wait_recv()
                g["prefix"][...] = g["prefix"][...] * g["decays"][q]

        first = iota2((half // 2, LANES), 1) < half

        def one(i, carry):
            t = g["prefix"][pl.ds(i, 1), :] * g["grad"][i]
            top, low = t[: half // 2], t[half // 2 :]
            h = 2 * i
            g["term"][h // x_size, h % x_size] = jnp.where(first, top, pltpu.roll(low, half, 1))
            g["term"][h // x_size, h % x_size + 1] = jnp.where(first, pltpu.roll(top, half, 1), low)
            return carry

        lax.fori_loop(0, pairs, one, 0)
        core_copy().start()

    def sum_core():
        core_copy().wait_recv()

        def one(n, carry):
            own = g["term"][n // x_size, n % x_size, pl.ds(pl.multiple_of(16 * c, 16), 16)]
            g["summed"][n // x_size, n % x_size] = own + g["core_in"][n // x_size, n % x_size]
            return carry

        lax.fori_loop(0, x_size * y_size, one, 0)
        for n in range(1, x_size):
            x_copy(n).start()

    def sum_x():
        for n in range(1, x_size):
            x_copy(n).wait_recv()
        for at in range(y_size):
            total = g["summed"][at, x]
            for n in range(1, x_size):
                total += g["x_in"][n - 1, at]
            g["x_sum"][at] = total
        for n in range(1, y_size):
            y_copy(n).start()

    def sum_y():
        for n in range(1, y_size):
            y_copy(n).wait_recv()
        total = g["x_sum"][y]
        for n in range(1, y_size):
            total += g["y_in"][n - 1]
        g["y_sum"][...] = total
        for n in range(4):
            to, copy = z_copy(n)

            @pl.when(to != z)
            def _():
                copy.start()

            @pl.when(to == z)
            def _():
                g["z_in"][z] = g["y_sum"][pl.ds(8 * (n % 2), 8)]

    def sum_z():
        @pl.when(gathers)
        def _():
            for q in range(seq_size):

                @pl.when(z != q)
                def _():
                    remote(
                        g["y_sum"].at[pl.ds(0, 8)], g["z_in"].at[q], g["zs"].at[0], g["zr"].at[q], {"seq": q}
                    ).wait_recv()

            total = g["z_in"][0]
            for q in range(1, seq_size):
                total += g["z_in"][q]
            g["z_sum"][...] = total
            last_copy().start()

    def finish():
        @pl.when(jnp.logical_not(gathers))
        def _():
            last_copy().wait_recv()
            g["z_sum"][...] = g["z_other"][...]

        total = g["z_sum"][...]
        total = jnp.where(z // 4 == 1, pltpu.roll(total, half, 1), total)
        total = jnp.where(c == 1, pltpu.roll(total, LANES - half // 2, 1), total)
        g["state_grad"][...] = total[:, : half // 2]

    stages = ((TERM_AT, make_terms), (CORE_AT, sum_core), (X_AT, sum_x), (Y_AT, sum_y), (Z_AT, sum_z), (LAST_AT, finish))
    finals = ("rec", "key", "val")

    def store(n, j):
        at = lanes_at(j)
        name = finals[n]
        return pltpu.make_async_copy(g[name + "_done"].at[:, at], g[name + "_out"].at[:, at], g["store_sem"].at[n, j])

    def tick(n, carry):
        jf = n - HOP * z
        jb = n - HOP * (last - z)
        j = n - HOP * jnp.maximum(z, last - z)

        @pl.when((z > 0) & (jf >= 0) & (jf < pairs))
        def _():
            forward(jf).wait_recv()

            @pl.when(z < last)
            def _():
                forward_on(jf)

        @pl.when((z < last) & (jb >= 0) & (jb < pairs))
        def _():
            backward(jb).wait_recv()

            @pl.when(z > 0)
            def _():
                backward_on(jb)

        @pl.when(n < pairs)
        def _():
            phase_two(n, g)

        for at, stage in stages:
            pl.when(n == at)(stage)

        @pl.when((j >= 0) & (j < pairs))
        def _():
            phase_three(j, g)
            for m in range(3):
                store(m, j).start()

        return carry

    lax.fori_loop(0, HOP * last + pairs, tick, 0)

    @pl.when(z < last)
    def _():
        lax.fori_loop(0, pairs, lambda j, s: (forward(j).wait_send(), s)[1], 0)

    @pl.when(z > 0)
    def _():
        lax.fori_loop(0, pairs, lambda j, s: (backward(j).wait_send(), s)[1], 0)

    for n in range(1, seq_size):

        @pl.when(z + n <= last)
        def _():
            decay_to(n).wait_send()

    core_copy().wait_send()
    for n in range(1, x_size):
        x_copy(n).wait_send()
    for n in range(1, y_size):
        y_copy(n).wait_send()
    for n in range(4):
        to, copy = z_copy(n)

        @pl.when(to != z)
        def _():
            copy.wait_send()

    @pl.when(gathers)
    def _():
        last_copy().wait_send()

    for m in range(3):
        lax.fori_loop(0, pairs, lambda j, s: (store(m, j).wait(), s)[1], 0)


def on_device(seq_size, dp_size, r, k, v, f, u, dy, initial):
    batch, tok, width = r.shape
    heads, size = u.shape
    pairs, half = width // LANES, LANES // 2
    x_size, y_size = X_SIZE, dp_size // (2 * X_SIZE)
    dma = lambda *n: pltpu.SemaphoreType.DMA(n)
    vmem = lambda *s: pltpu.VMEM(s, F32)
    scratch = {n: pltpu.VMEM((tok, width), BF16) for n in ("r", "k", "v", "f", "dy", "rec_done", "key_done", "val_done")}
    scratch |= {n: vmem(tok, width) for n in ("upto", "before", "early", "tail", "rec", "key", "val")}
    scratch |= {n: vmem(pairs, half, LANES) for n in ("state", "grad", "state_in", "grad_in", "state_out", "grad_out")}
    scratch |= {
        "initial": vmem(size, width),
        "decay": vmem(pairs, LANES),
        "prefix": vmem(pairs, LANES),
        "decays": vmem(seq_size, pairs, LANES),
        "term": vmem(y_size, x_size, half // 2, LANES),
        "core_in": vmem(y_size, x_size, half // 4, LANES),
        "summed": vmem(y_size, x_size, half // 4, LANES),
        "x_in": vmem(x_size - 1, y_size, half // 4, LANES),
        "x_sum": vmem(y_size, half // 4, LANES),
        "y_in": vmem(max(y_size - 1, 1), half // 4, LANES),
        "y_sum": vmem(half // 4, LANES),
        "z_in": vmem(seq_size, 8, LANES),
        "z_sum": vmem(8, LANES),
        "z_other": vmem(8, LANES),
        "load_sem": dma(6),
        "store_sem": dma(3, pairs),
        "fs": dma(pairs),
        "fr": dma(pairs),
        "bs": dma(pairs),
        "br": dma(pairs),
        "ds": dma(seq_size),
        "dr": dma(seq_size),
        "cs": dma(2),
        "cr": dma(2),
        "xs": dma(x_size),
        "xr": dma(x_size),
        "ys": dma(y_size),
        "yr": dma(y_size),
        "zs": dma(4),
        "zr": dma(seq_size),
    }
    names = ("r_hbm", "k_hbm", "v_hbm", "f_hbm", "dy_hbm", "u", "initial_hbm") + OUT + tuple(scratch)
    anywhere = pl.BlockSpec(memory_space=pl.ANY)
    inside = pl.BlockSpec(memory_space=pltpu.VMEM)
    tokens = jax.ShapeDtypeStruct((tok, width), BF16)
    outs = pl.pallas_call(
        functools.partial(kernel, seq_size, dp_size, names),
        out_shape=[tokens] * 3 + [jax.ShapeDtypeStruct((size // seq_size, half // 2), F32)],
        in_specs=[anywhere] * 5 + [inside, anywhere],
        out_specs=[anywhere] * 3 + [inside],
        scratch_shapes=list(scratch.values()),
        compiler_params=pltpu.CompilerParams(vmem_limit_bytes=56 << 20, collective_id=0, has_side_effects=True),
    )(*(a.reshape(tok, width) for a in (r, k, v, f, dy)), u, initial.T)
    return tuple(o.reshape(batch, tok, width) for o in outs[:3]) + (outs[3].T,)


def solution(mesh):
    rows = P("dp", "seq", None)
    return jax.shard_map(
        functools.partial(on_device, mesh.shape["seq"], mesh.shape["dp"]),
        mesh=mesh,
        in_specs=(rows, rows, rows, rows, P(), rows, P()),
        out_specs=(rows, rows, rows, P("dp", "seq")),
        check_vma=False,
    )
```

```python
import functools
from types import SimpleNamespace

import jax
import jax.numpy as jnp
from jax import lax
from jax.experimental import pallas as pl
from jax.experimental.pallas import tpu as pltpu
from jax.sharding import PartitionSpec as P

F32 = jnp.float32
BF16 = jnp.bfloat16
LANES = 128
BLOCK = 32


def dot_nn(a, b):
    return lax.dot_general(a, b, (((1,), (0,)), ((), ())), preferred_element_type=F32)


def dot_nt(a, b):
    return lax.dot_general(a, b, (((1,), (1,)), ((), ())), preferred_element_type=F32)


def dot_tn(a, b):
    return lax.dot_general(a, b, (((0,), (0,)), ((), ())), preferred_element_type=F32)


def halves(x):
    hi = x.astype(BF16)
    return hi, (x - hi.astype(F32)).astype(BF16)


def thirds(x):
    hi = x.astype(BF16)
    rest = x - hi.astype(F32)
    mid = rest.astype(BF16)
    return hi, mid, (rest - mid.astype(F32)).astype(BF16)


def iota2(shape, dim):
    return lax.broadcasted_iota(jnp.int32, shape, dim)


def per_head_halves(x, heads):
    hi, lo = halves(x)
    return jnp.concatenate(
        [
            jnp.concatenate([hi * heads[0], lo * heads[0]], axis=1),
            jnp.concatenate([hi * heads[1], lo * heads[1]], axis=1),
        ],
        axis=0,
    )


def per_head_rows(x, heads):
    return jnp.concatenate([x * heads[0], x * heads[1]], axis=0)


def folded(x):
    return x[:, :LANES] + x[:, LANES:]


def rows_of(parts):
    return jnp.concatenate([jnp.broadcast_to(p, (BLOCK, LANES)) for p in parts], axis=0)


def decay_sums(f_pair, tri):
    log_w = -jnp.exp(f_pair.astype(F32))
    hi, mid, lo = thirds(log_w)
    sums = dot_nn(tri, jnp.concatenate([hi, mid, lo], axis=1))
    upto = sums[:, :LANES] + (sums[:, LANES : 2 * LANES] + sums[:, 2 * LANES :])
    return upto, upto - log_w


def totals_of(upto):
    return [upto[b * BLOCK + BLOCK - 1 : (b + 1) * BLOCK] for b in range(upto.shape[0] // BLOCK)]


def shard_sums(upto):
    t = totals_of(upto)
    zero = jnp.zeros_like(t[0])
    ahead = [zero, t[0], t[0] + t[1], t[0] + t[1] + t[2]]
    behind = [t[1] + t[2] + t[3], t[2] + t[3], t[3], zero]
    return t, ahead, behind


def lanes_at(i):
    return pl.ds(pl.multiple_of(i * LANES, LANES), LANES)


def rows_at(i, count):
    return pl.ds(pl.multiple_of(i * count, count), count)


def prepare(refs):
    tok = refs.tri.shape[0]
    row, col = iota2((tok, tok), 0), iota2((tok, tok), 1)
    same = row // BLOCK == col // BLOCK
    refs.tri[...] = jnp.where((col <= row) & same, 1.0, 0.0).astype(BF16)
    row, col = iota2((tok, 2 * tok), 0), iota2((tok, 2 * tok), 1) % tok
    same = row // BLOCK == col // BLOCK
    refs.lower[...] = jnp.where((col < row) & same, 1.0, 0.0).astype(BF16)
    upper = jnp.where((col > row) & same, 1.0, 0.0)
    refs.upper[...] = upper.astype(BF16)
    refs.upper_f[...] = upper
    row, col = iota2((tok // 2, 2 * tok), 0), iota2((tok // 2, 2 * tok), 1) % tok
    later, earlier = 2 * (row // BLOCK) + 1, 2 * (row // BLOCK)
    refs.lower_1[...] = jnp.where(col // BLOCK == later - 1, 1.0, 0.0).astype(BF16)
    upper = jnp.where(col // BLOCK == earlier + 1, 1.0, 0.0)
    refs.upper_1[...] = upper.astype(BF16)
    refs.upper_1f[...] = upper
    first = iota2((tok, LANES), 1) < LANES // 2
    refs.heads[0] = jnp.where(first, 1.0, 0.0).astype(BF16)
    refs.heads[1] = jnp.where(first, 0.0, 1.0).astype(BF16)
    same = (iota2((2 * LANES, LANES), 0) % LANES < LANES // 2) == (iota2((2 * LANES, LANES), 1) < LANES // 2)
    refs.ones[...] = jnp.where(same, 1.0, 0.0).astype(BF16)


def shard_decay(i, refs):
    rates = jnp.exp(refs.f[:, lanes_at(i)].astype(F32))
    refs.decay[pl.ds(i, 1), :] = jnp.exp(-jnp.sum(rates, axis=0, keepdims=True))


def phase_one(pairs, refs):
    first = iota2((LANES // 2, LANES), 1) < LANES // 2
    tri = refs.tri[...]
    done = []
    for i in pairs:
        at = lanes_at(i)
        upto, before = decay_sums(refs.f[:, at], tri)
        t, ahead, behind = shard_sums(upto)
        early = jnp.exp(before + rows_of(ahead))
        tail = jnp.exp(rows_of([a + b for a, b in zip(t, behind)]) - upto)

        def increment(x, scaled):
            hi, lo = halves(scaled)
            both = folded(dot_tn(x, jnp.concatenate([hi, lo], axis=1)))
            return jnp.where(first, both[: LANES // 2], both[LANES // 2 :])

        state = increment(refs.v[:, at], refs.k[:, at].astype(F32) * tail)
        grad = increment(refs.dy[:, at], refs.r[:, at].astype(F32) * early)
        done.append((i, at, upto, before, early, tail, state, grad))
    for i, at, upto, before, early, tail, state, grad in done:
        refs.upto[:, at] = upto
        refs.before[:, at] = before
        refs.early[:, at] = early
        refs.tail[:, at] = tail
        refs.state[i] = state
        refs.grad[i] = grad


def picked(x, blocks):
    return jnp.concatenate([x[b * BLOCK : (b + 1) * BLOCK] for b in blocks], axis=0)


def spread(parts, values, blocks):
    for n, b in enumerate(blocks):
        parts[b] = parts[b] + values[n * BLOCK : (n + 1) * BLOCK]


def only(x, blocks):
    zero = jnp.zeros((BLOCK, x.shape[1]), x.dtype)
    count = x.shape[0] // BLOCK
    return jnp.concatenate([x[b * BLOCK : (b + 1) * BLOCK] if b % 4 in blocks else zero for b in range(count)], axis=0)


ALL, ODD, EVEN, LATE, FIRST = (0, 1, 2, 3), (1, 3), (0, 2), (2, 3), (0, 1)


def levels_of(x, heads, inner, outer, last, cut):
    made = [per_head_halves(x * scale, heads) for scale in (inner, outer, last)]
    made[2] = only(made[2], cut)
    return made


def level_product(hi, lo, operand):
    return folded(dot_nn(hi, operand)) + dot_nn(lo, operand[:, :LANES])


def cross_product(k_heads, r_heads, blocks):
    both = picked(k_heads[:LANES] + k_heads[LANES:], blocks)
    rows = both.shape[0]
    stacked = jnp.concatenate([both[:, :LANES], both[:, LANES:]], axis=0)
    main = dot_nt(stacked, r_heads[:, :LANES])
    return main[:rows] + main[rows:] + dot_nt(both[:, :LANES], r_heads[:, LANES:])


def phase_two(i, refs):
    at = lanes_at(i)
    r, k = refs.r[:, at].astype(F32), refs.k[:, at].astype(F32)
    v, dy = refs.v[:, at], refs.dy[:, at]
    upto, before = refs.upto[:, at], refs.before[:, at]
    heads = [refs.heads[0], refs.heads[1]]
    t = totals_of(upto)
    whole = rows_of(t)
    half = 0.5 * whole
    early_0, tail_0 = jnp.exp(before - half), jnp.exp(half - upto)
    early_1, tail_1 = jnp.exp(before), jnp.exp(whole - upto)
    zero = jnp.zeros_like(t[0])
    early_2 = early_1 * jnp.exp(rows_of([zero, zero, zero, t[2]]))
    tail_2 = tail_1 * jnp.exp(rows_of([t[1], zero, zero, zero]))
    k_heads = levels_of(k, heads, tail_0, tail_1, tail_2, FIRST)
    r_heads = levels_of(r, heads, early_0, early_1, early_2, LATE)
    dy_heads = per_head_rows(dy, heads)

    hi, lo = halves(dot_nt(dy, per_head_rows(v, heads)))
    lower, lower_1 = refs.lower[...], refs.lower_1[...]
    inner = level_product(hi * lower, lo * lower, k_heads[0]) * early_0
    rec = [inner[b * BLOCK : (b + 1) * BLOCK] for b in ALL]
    outer = level_product(picked(hi, ODD) * lower_1, picked(lo, ODD) * lower_1, k_heads[1])
    spread(rec, outer * picked(early_1, ODD), ODD)
    spread(rec, level_product(picked(hi, LATE), picked(lo, LATE), k_heads[2]) * picked(early_2, LATE), LATE)

    hi, lo = halves(dot_nt(v, dy_heads))
    upper, upper_1 = refs.upper[...], refs.upper_1[...]
    inner = level_product(hi * upper, lo * upper, r_heads[0]) * tail_0
    key = [inner[b * BLOCK : (b + 1) * BLOCK] for b in ALL]
    outer = level_product(picked(hi, EVEN) * upper_1, picked(lo, EVEN) * upper_1, r_heads[1])
    spread(key, outer * picked(tail_1, EVEN), EVEN)
    spread(key, level_product(picked(hi, FIRST), picked(lo, FIRST), r_heads[2]) * picked(tail_2, FIRST), FIRST)

    inner = jnp.where(refs.upper_f[...] > 0.0, cross_product(k_heads[0], r_heads[0], ALL), 0.0)
    cross = [inner[b * BLOCK : (b + 1) * BLOCK] for b in ALL]
    spread(cross, cross_product(k_heads[1], r_heads[1], EVEN) * refs.upper_1f[...], EVEN)
    spread(cross, cross_product(k_heads[2], r_heads[2], FIRST), FIRST)
    hi, lo = halves(jnp.concatenate(cross, axis=0))
    val = dot_nn(hi, dy_heads) + dot_nn(lo, dy_heads)

    boost = jnp.concatenate([refs.u[pl.ds(2 * i, 1), :], refs.u[pl.ds(2 * i + 1, 1), :]], axis=1)
    dy_f = dy.astype(F32)
    own_r, own_k = r * boost, k * boost
    ones = refs.ones[...]
    scalar = dot_nn(jnp.concatenate(halves(v.astype(F32) * dy_f), axis=1), ones)
    factor = dot_nn(jnp.concatenate(halves(own_r * k), axis=1), ones)
    refs.rec[:, at] = jnp.concatenate(rec, axis=0) + own_k * scalar
    refs.key[:, at] = jnp.concatenate(key, axis=0) + own_r * scalar
    refs.val[:, at] = val + factor * dy_f


def phase_three(i, refs):
    at = lanes_at(i)
    v, dy = refs.v[:, at], refs.dy[:, at]
    early, tail = refs.early[:, at], refs.tail[:, at]
    half = LANES // 2
    heads = [refs.heads[0, :half], refs.heads[1, :half]]
    state_in = per_head_halves(refs.state_in[i], heads)
    grad_in = per_head_halves(refs.grad_in[i], heads)
    grad_hi, grad_lo = grad_in[:, :LANES], grad_in[:, LANES:]
    k_hi, k_lo = halves(refs.k[:, at].astype(F32) * tail)
    both = jnp.concatenate([k_hi, k_lo], axis=1)
    rec = refs.rec[:, at] + early * folded(dot_nn(dy, state_in))
    key = refs.key[:, at] + tail * folded(dot_nn(v, grad_in))
    val = refs.val[:, at] + (dot_nt(both, jnp.concatenate([grad_hi, grad_hi], axis=1)) + dot_nt(k_hi, grad_lo))
    refs.rec_out[:, at] = rec.astype(BF16)
    refs.key_out[:, at] = key.astype(BF16)
    refs.val_out[:, at] = val.astype(BF16)


X_SIZE = 4
HOP = 5
TERM_AT, CORE_AT, X_AT, Y_AT, Z_AT, LAST_AT = 3, 10, 21, 32, 42, 50
TERM_TICKS = 4
EVERY = 2
MIDDLE_FIRST, MIDDLE_AFTER = 10, 36
EARLY = 2

OUT = ("rec_out", "key_out", "val_out", "state_grad")


def kernel(seq_size, dp_size, names, *all_refs):
    g = SimpleNamespace(**dict(zip(names, all_refs)))
    pairs = g.state.shape[0]
    half = LANES // 2
    x_size, y_size = X_SIZE, dp_size // (2 * X_SIZE)
    z, d = lax.axis_index("seq"), lax.axis_index("dp")
    c = d % 2
    x = (d // 2) % x_size
    y = d // (2 * x_size)
    last = seq_size - 1

    def chip(x_at, y_at, c_at):
        return {"dp": (y_at * x_size + x_at) * 2 + c_at}

    ways = ((g.f_hbm, g.f), (g.k_hbm, g.k), (g.v_hbm, g.v), (g.r_hbm, g.r), (g.dy_hbm, g.dy), (g.u_hbm, g.u))
    loads = [pltpu.make_async_copy(src, dst, g.load_sem.at[at]) for at, (src, dst) in enumerate(ways)]
    for load in loads:
        load.start()
    load_initial = pltpu.make_async_copy(g.initial_hbm, g.initial, g.load_sem.at[6])

    @pl.when(z == 0)
    def _():
        load_initial.start()

    barrier = pltpu.get_barrier_semaphore()
    peers = [{"seq": (z + n) % seq_size} for n in range(1, seq_size)]
    peers += [chip((x + n) % x_size, y, c) for n in range(1, x_size)]
    peers += [chip(x, (y + n) % y_size, c) for n in range(1, y_size)]
    peers += [chip(x, y, 1 - c)]
    for peer in peers:
        pl.semaphore_signal(barrier, inc=1, device_id=peer, device_id_type=pl.DeviceIdType.MESH)

    def remote(src, dst, send, recv, to):
        return pltpu.make_async_remote_copy(
            src_ref=src, dst_ref=dst, send_sem=send, recv_sem=recv, device_id=to, device_id_type=pl.DeviceIdType.MESH
        )

    def forward(j):
        to = {"seq": (z + 1) % seq_size}
        return remote(g.state_out.at[j], g.state_in.at[j], g.fs.at[0], g.fr.at[j], to)

    def backward(j):
        to = {"seq": (z + last) % seq_size}
        return remote(g.grad_out.at[j], g.grad_in.at[j], g.bs.at[0], g.br.at[j], to)

    def forward_on(j):
        g.state_out[j] = g.decay[pl.ds(j, 1), :] * g.state_in[j] + g.state[j]
        forward(j).start()

    def backward_on(j):
        g.grad_out[j] = g.decay[pl.ds(j, 1), :] * g.grad_in[j] + g.grad[j]
        backward(j).start()

    prepare(g)
    loads[0].wait()
    lax.fori_loop(0, pairs, lambda i, s: (shard_decay(i, g), s)[1], 0)
    for load in loads[1:]:
        load.wait()

    def one_step(i, carry):
        phase_one([2 * i, 2 * i + 1], g)
        return carry

    def send_first(i):
        @pl.when(z == 0)
        def _():
            g.state_in[i] = g.initial[:, lanes_at(i)]
            forward_on(i)

        @pl.when(z == last)
        def _():
            g.grad_in[i] = jnp.zeros((half, LANES), F32)
            backward_on(i)

    def start_step(i, carry):
        phase_one([2 * i, 2 * i + 1], g)
        send_first(2 * i)
        send_first(2 * i + 1)
        return carry

    def send_step(i, carry):
        send_first(i)
        return carry

    lax.fori_loop(0, EARLY, one_step, 0)

    @pl.when(z == 0)
    def _():
        load_initial.wait()

    def decay_to(n):
        return remote(g.decay, g.decays.at[z], g.ds.at[n - 1], g.dr.at[z], {"seq": (z + n) % seq_size})

    pl.semaphore_wait(barrier, len(peers))
    for n in range(1, seq_size):

        @pl.when(z + n <= last)
        def _():
            decay_to(n).start()

    lax.fori_loop(0, 2 * EARLY, send_step, 0)
    lax.fori_loop(EARLY, pairs // 2, start_step, 0)

    def core_copy():
        return remote(
            g.term.at[:, :, pl.ds(pl.multiple_of(16 * (1 - c), 16), 16)],
            g.core_in,
            g.cs.at[0],
            g.cr.at[0],
            chip(x, y, 1 - c),
        )

    def x_copy(n):
        to = (x + n) % x_size
        return remote(g.summed.at[:, to], g.x_in.at[n - 1], g.xs.at[n - 1], g.xr.at[n - 1], chip(to, y, c))

    def y_copy(n):
        to = (y + n) % y_size
        return remote(g.x_sum.at[to], g.y_in.at[n - 1], g.ys.at[n - 1], g.yr.at[n - 1], chip(x, to, c))

    def z_copy(n):
        b, hi = n % 2, n // 2
        to = 2 * c + b + 4 * hi
        return to, remote(g.y_sum.at[pl.ds(8 * b, 8)], g.z_in.at[z], g.zs.at[n], g.zr.at[z], {"seq": to})

    def last_copy():
        return remote(g.z_sum, g.z_other, g.cs.at[1], g.cr.at[1], chip(x, y, 1 - c))

    gathers = (z % 4) // 2 == c

    def make_prefix():
        g.prefix[...] = jnp.ones((pairs, LANES), F32)
        for q in range(last):

            @pl.when(q < z)
            def _():
                remote(g.decay, g.decays.at[q], g.ds.at[0], g.dr.at[q], {"seq": z}).wait_recv()
                g.prefix[...] = g.prefix[...] * g.decays[q]

    first = iota2((half // 2, LANES), 1) < half

    def make_term(i):
        t = g.prefix[pl.ds(i, 1), :] * g.grad[i]
        top, low = t[: half // 2], t[half // 2 :]
        h = 2 * i
        g.term[h // x_size, h % x_size] = jnp.where(first, top, pltpu.roll(low, half, 1))
        g.term[h // x_size, h % x_size + 1] = jnp.where(first, pltpu.roll(top, half, 1), low)

    def sum_core():
        core_copy().wait_recv()

        def one(n, carry):
            own = g.term[n // x_size, n % x_size, pl.ds(pl.multiple_of(16 * c, 16), 16)]
            g.summed[n // x_size, n % x_size] = own + g.core_in[n // x_size, n % x_size]
            return carry

        lax.fori_loop(0, x_size * y_size, one, 0)
        for n in range(1, x_size):
            x_copy(n).start()

    def sum_x():
        for n in range(1, x_size):
            x_copy(n).wait_recv()
        for at in range(y_size):
            total = g.summed[at, x]
            for n in range(1, x_size):
                total += g.x_in[n - 1, at]
            g.x_sum[at] = total
        for n in range(1, y_size):
            y_copy(n).start()

    def sum_y():
        for n in range(1, y_size):
            y_copy(n).wait_recv()
        total = g.x_sum[y]
        for n in range(1, y_size):
            total += g.y_in[n - 1]
        g.y_sum[...] = total
        for n in range(4):
            to, copy = z_copy(n)

            @pl.when(to != z)
            def _():
                copy.start()

            @pl.when(to == z)
            def _():
                g.z_in[z] = g.y_sum[pl.ds(8 * (n % 2), 8)]

    def sum_z():
        @pl.when(gathers)
        def _():
            for q in range(seq_size):

                @pl.when(z != q)
                def _():
                    remote(
                        g.y_sum.at[pl.ds(0, 8)], g.z_in.at[q], g.zs.at[0], g.zr.at[q], {"seq": q}
                    ).wait_recv()

            total = g.z_in[0]
            for q in range(1, seq_size):
                total += g.z_in[q]
            g.z_sum[...] = total
            last_copy().start()

    def finish():
        @pl.when(jnp.logical_not(gathers))
        def _():
            last_copy().wait_recv()
            g.z_sum[...] = g.z_other[...]

        total = g.z_sum[...]
        total = jnp.where(z // 4 == 1, pltpu.roll(total, half, 1), total)
        total = jnp.where(c == 1, pltpu.roll(total, LANES - half // 2, 1), total)
        g.state_grad[...] = total[:, : half // 2]

    stages = ((TERM_AT, make_prefix), (TERM_AT + TERM_TICKS, lambda: core_copy().start()), (CORE_AT, sum_core), (X_AT, sum_x), (Y_AT, sum_y), (Z_AT, sum_z), (LAST_AT, finish))
    def tick(n, carry):
        jf = n - HOP * z
        jb = n - HOP * (last - z)
        far = HOP * jnp.maximum(z, last - z)
        middle = (2 * z == last - 1) | (2 * z == last + 1)
        after = (n - MIDDLE_AFTER) // EVERY
        beat = (n - MIDDLE_AFTER) % EVERY == 0
        early_unit = middle & (n < MIDDLE_FIRST)
        late_unit = middle & (n >= MIDDLE_AFTER) & beat & (MIDDLE_FIRST + after < pairs)
        outer_unit = jnp.logical_not(middle) & beat & (n < EVERY * pairs)
        unit = jnp.where(middle, jnp.where(n < MIDDLE_FIRST, n, MIDDLE_FIRST + after), n // EVERY)
        j = jnp.where(late_unit, MIDDLE_FIRST + after, n - far)
        takes = late_unit | ((n >= far) & (n - far < jnp.where(middle, MIDDLE_FIRST, pairs)))

        @pl.when((z > 0) & (jf >= 0) & (jf < pairs))
        def _():
            forward(jf).wait_recv()

            @pl.when(z < last)
            def _():
                forward_on(jf)

        @pl.when((z < last) & (jb >= 0) & (jb < pairs))
        def _():
            backward(jb).wait_recv()

            @pl.when(z > 0)
            def _():
                backward_on(jb)

        @pl.when(early_unit | late_unit | outer_unit)
        def _():
            phase_two(unit, g)

        for at, stage in stages:
            pl.when(n == at)(stage)

        @pl.when((n >= TERM_AT) & (n < TERM_AT + TERM_TICKS))
        def _():
            for m in range(pairs // TERM_TICKS):
                make_term((n - TERM_AT) * (pairs // TERM_TICKS) + m)

        @pl.when(takes)
        def _():
            phase_three(j, g)

        return carry

    lax.fori_loop(0, HOP * last + pairs, tick, 0)

    @pl.when(z < last)
    def _():
        remote(g.state_out, g.state_in, g.fs.at[0], g.fr.at[0], {"seq": (z + 1) % seq_size}).wait_send()

    @pl.when(z > 0)
    def _():
        remote(g.grad_out, g.grad_in, g.bs.at[0], g.br.at[0], {"seq": (z + last) % seq_size}).wait_send()

    for n in range(1, seq_size):

        @pl.when(z + n <= last)
        def _():
            decay_to(n).wait_send()

    core_copy().wait_send()
    for n in range(1, x_size):
        x_copy(n).wait_send()
    for n in range(1, y_size):
        y_copy(n).wait_send()
    for n in range(4):
        to, copy = z_copy(n)

        @pl.when(to != z)
        def _():
            copy.wait_send()

    @pl.when(gathers)
    def _():
        last_copy().wait_send()


def store_kernel(count, *refs):
    ins, outs, sem = refs[:count], refs[count : 2 * count], refs[2 * count]
    puts = [pltpu.make_async_copy(ins[n], outs[n], sem.at[n]) for n in range(count)]
    for put in puts:
        put.start()
    for put in puts:
        put.wait()


def stored(arrays):
    count = len(arrays)
    return pl.pallas_call(
        functools.partial(store_kernel, count),
        out_shape=[jax.ShapeDtypeStruct(a.shape, a.dtype) for a in arrays],
        in_specs=[pl.BlockSpec(memory_space=pltpu.VMEM)] * count,
        out_specs=[pl.BlockSpec(memory_space=pl.ANY)] * count,
        scratch_shapes=[pltpu.SemaphoreType.DMA((count,))],
        compiler_params=pltpu.CompilerParams(vmem_limit_bytes=24 << 20),
    )(*arrays)


def in_hbm(array):
    return pltpu.with_memory_space_constraint(array, pltpu.HBM)


def on_device(seq_size, dp_size, r, k, v, f, u, dy, initial):
    batch, tok, width = r.shape
    heads, size = u.shape
    pairs, half = width // LANES, LANES // 2
    x_size, y_size = X_SIZE, dp_size // (2 * X_SIZE)
    dma = lambda *n: pltpu.SemaphoreType.DMA(n)
    vmem = lambda *s: pltpu.VMEM(s, F32)
    scratch = dict(
        r=pltpu.VMEM((tok, width), BF16),
        k=pltpu.VMEM((tok, width), BF16),
        v=pltpu.VMEM((tok, width), BF16),
        f=pltpu.VMEM((tok, width), BF16),
        dy=pltpu.VMEM((tok, width), BF16),
        upto=vmem(tok, width),
        before=vmem(tok, width),
        early=vmem(tok, width),
        tail=vmem(tok, width),
        rec=vmem(tok, width),
        key=vmem(tok, width),
        val=vmem(tok, width),
        state=vmem(pairs, half, LANES),
        grad=vmem(pairs, half, LANES),
        state_in=vmem(pairs, half, LANES),
        grad_in=vmem(pairs, half, LANES),
        state_out=vmem(pairs, half, LANES),
        grad_out=vmem(pairs, half, LANES),
        initial=vmem(size, width),
        u=vmem(heads, size),
        tri=pltpu.VMEM((tok, tok), BF16),
        lower=pltpu.VMEM((tok, 2 * tok), BF16),
        upper=pltpu.VMEM((tok, 2 * tok), BF16),
        upper_f=vmem(tok, 2 * tok),
        lower_1=pltpu.VMEM((tok // 2, 2 * tok), BF16),
        upper_1=pltpu.VMEM((tok // 2, 2 * tok), BF16),
        upper_1f=vmem(tok // 2, 2 * tok),
        heads=pltpu.VMEM((2, tok, LANES), BF16),
        ones=pltpu.VMEM((2 * LANES, LANES), BF16),
        decay=vmem(pairs, LANES),
        prefix=vmem(pairs, LANES),
        decays=vmem(seq_size, pairs, LANES),
        term=vmem(y_size, x_size, half // 2, LANES),
        core_in=vmem(y_size, x_size, half // 4, LANES),
        summed=vmem(y_size, x_size, half // 4, LANES),
        x_in=vmem(x_size - 1, y_size, half // 4, LANES),
        x_sum=vmem(y_size, half // 4, LANES),
        y_in=vmem(max(y_size - 1, 1), half // 4, LANES),
        y_sum=vmem(half // 4, LANES),
        z_in=vmem(seq_size, 8, LANES),
        z_sum=vmem(8, LANES),
        z_other=vmem(8, LANES),
        load_sem=dma(7),
        fs=dma(1),
        fr=dma(pairs),
        bs=dma(1),
        br=dma(pairs),
        ds=dma(seq_size),
        dr=dma(seq_size),
        cs=dma(2),
        cr=dma(2),
        xs=dma(x_size),
        xr=dma(x_size),
        ys=dma(y_size),
        yr=dma(y_size),
        zs=dma(4),
        zr=dma(seq_size),
    )
    names = ("r_hbm", "k_hbm", "v_hbm", "f_hbm", "dy_hbm", "u_hbm", "initial_hbm") + OUT + tuple(scratch)
    anywhere = pl.BlockSpec(memory_space=pl.ANY)
    inside = pl.BlockSpec(memory_space=pltpu.VMEM)
    tokens = jax.ShapeDtypeStruct((tok, width), BF16)
    outs = pl.pallas_call(
        functools.partial(kernel, seq_size, dp_size, names),
        out_shape=[tokens] * 3 + [jax.ShapeDtypeStruct((size // seq_size, half // 2), F32)],
        in_specs=[anywhere] * 7,
        out_specs=[inside] * 4,
        scratch_shapes=list(scratch.values()),
        compiler_params=pltpu.CompilerParams(vmem_limit_bytes=24 << 20, collective_id=0, has_side_effects=True),
    )(*(in_hbm(a) for a in (*(a.reshape(tok, width) for a in (r, k, v, f, dy)), u, initial.T)))
    outs = stored(outs)
    return tuple(o.reshape(batch, tok, width) for o in outs[:3]) + (outs[3].T,)


def solution(mesh):
    rows = P("dp", "seq", None)
    return jax.shard_map(
        functools.partial(on_device, mesh.shape["seq"], mesh.shape["dp"]),
        mesh=mesh,
        in_specs=(rows, rows, rows, rows, P(), rows, P()),
        out_specs=(rows, rows, rows, P("dp", "seq")),
        check_vma=False,
    )
```
